128 devices in a mesh: band: 8 (over y, x_lo), chan: 16 (over x_hi, z, core).
Axes of the slice: x: 4 (x_hi: 2, x_lo: 2; x = x_hi * 2 + x_lo), y: 4, z: 4, core: 2. Of those that a mesh axis runs over, the one named last changes fastest.
Arguments:
- coeffs: bfloat16 [2, 8, 1024, 8192], P(None, None, 'chan', 'band'), may hold values from -1100 to 1100, as said below
Outputs:
- coherence: float32 [1024, 1024], P('chan', 'band')
The draws below stay inside these ranges and needn't reach their ends.
Inputs may be any that keep to these rules, and one draw needn't show every extreme that they name: `coeffs`: finite real and imaginary parts.
All inputs are finite; a program needn't handle non-finite values.
Results may differ from the reference program's by a relative error of at most 0.0003.
Values may be sent and summed in bfloat16 or wider, within the bound.
No kernel may reach another device: no remote copies, remote signals or barrier semaphores. Data moves between devices by JAX's collectives and lax.ppermute only.
A program may use at most 192 MiB of HBM per device.

```python
import jax
import jax.numpy as jnp
from jax import lax

C = 1024
K = 8
W = 16
BINS = 8192


def draw_coeffs(key, part):
    noise_key = jax.random.fold_in(jax.random.fold_in(key, 17), 0)
    noise = jnp.clip(jax.random.normal(noise_key, (2, K, C, BINS), jnp.float32), -6.0, 6.0)
    values = noise
    return values.astype(jnp.bfloat16)


def setup_inputs(seed: int = 0) -> dict:
    splits = jax.random.split(jax.random.key(seed), 2)
    return {
        "coeffs": draw_coeffs(jax.random.fold_in(splits[1], 71), 0),
    }


epsilon = 1e-6


def band_term(total, block):
    width = block.shape[2]
    flat = block.transpose(2, 0, 1, 3).reshape(width, -1)
    paired = jnp.stack((block[1], -block[0]), axis=0).transpose(2, 0, 1, 3).reshape(width, -1)
    real_part = jnp.dot(flat, flat.T, preferred_element_type=jnp.float32)
    imag_part = jnp.dot(paired, flat.T, preferred_element_type=jnp.float32)
    wide = flat.astype(jnp.float32)
    power = jnp.sum(wide * wide, axis=1) + epsilon
    coh_band = (real_part * real_part + imag_part * imag_part) / (power[:, None] * power[None, :])
    return total + coh_band, None


def reference(coeffs):
    num_bands = BINS // W
    width = coeffs.shape[2]
    blocks = coeffs.reshape(2, K, width, num_bands, W)
    blocks = jnp.moveaxis(blocks, 3, 0)
    total, unused = lax.scan(band_term, jnp.zeros((width, width), jnp.float32), blocks)
    rows = lax.broadcasted_iota(jnp.int32, (width, width), 0)
    cols = lax.broadcasted_iota(jnp.int32, (width, width), 1)
    total = jnp.where(rows == cols, jnp.float32(0.0), total)
    return total * jnp.float32(W * K / num_bands)
```

```python
import jax
import jax.numpy as jnp
from jax import lax
from jax.experimental import pallas as pl
from jax.experimental.pallas import tpu as pltpu
from jax.sharding import Mesh, PartitionSpec as P

K = 8
W = 16
EPS = 1e-06


def turn_kernel(x_ref, o_ref):
    tiles = x_ref.shape[3] // 128
    for t in range(tiles):
        re = x_ref[0, 0, :, t * 128 : (t + 1) * 128]
        im = x_ref[1, 0, :, t * 128 : (t + 1) * 128]
        both = jnp.concatenate((re, im), axis=0).T
        o_ref[2 * t, 0] = both[:64]
        o_ref[2 * t + 1, 0] = both[64:]


def turned(coeffs):
    width, bins = coeffs.shape[2:]
    return pl.pallas_call(
        turn_kernel,
        grid=(K,),
        in_specs=[pl.BlockSpec((2, 1, width, bins), lambda k: (0, k, 0, 0))],
        out_specs=pl.BlockSpec((bins // 64, 1, 64, 128), lambda k: (0, k, 0, 0)),
        out_shape=jax.ShapeDtypeStruct((bins // 64, K, 64, 128), jnp.bfloat16),
    )(coeffs)


BANDS = 4


def pair_kernel(core_ref, x_ref, own_ref, other_ref, right, left, row_inv, col_inv):
    core = core_ref[0]
    low = lax.broadcasted_iota(jnp.int32, (BANDS * W, 128), 1) < 64
    for s in range(8):
        lanes = slice(s * 128, (s + 1) * 128)
        for k in range(K):
            a = x_ref[2 * s, k]
            b = x_ref[2 * s + 1, k]
            a_turned = jnp.concatenate((a[:, 64:], a[:, :64]), axis=1)
            b_turned = jnp.concatenate((b[:, 64:], b[:, :64]), axis=1)
            re = jnp.where(low, a, b_turned)
            im = jnp.where(low, a_turned, b)
            for n in range(BANDS):
                right[n, k * W : (k + 1) * W, lanes] = re[n * W : (n + 1) * W]
                right[n, 128 + k * W : 128 + (k + 1) * W, lanes] = im[n * W : (n + 1) * W]

    def prepare(i, carry):
        n = i // 8
        s = i % 8
        block = right[n, :, pl.ds(pl.multiple_of(s * 128, 128), 128)]
        wide = block.astype(jnp.float32)
        power = jnp.sum(wide * wide, axis=0, keepdims=True) + EPS
        inv = 1.0 / power
        row_inv[n, :, pl.ds(pl.multiple_of(s * 128, 128), 128)] = jnp.broadcast_to(inv, (8, 128))
        rows = pl.ds(pl.multiple_of(s * 128, 128), 128)
        turned = block.T
        left[0, n, rows, :] = turned
        left[1, n, rows, 0:128] = turned[:, 128:]
        left[1, n, rows, 128:256] = -turned[:, :128]
        col_inv[n, rows, :] = jnp.broadcast_to(inv, (128, 128)).T
        return carry

    lax.fori_loop(0, BANDS * 8, prepare, 0)

    def tile(s, carry):
        for half in range(2):
            out_ref = (own_ref, other_ref)[half]
            c = core if half == 0 else 1 - core
            rows = pl.ds(pl.multiple_of(s * 128 + c * 64, 64), 64)
            for j in range(4):
                cols = slice(j * 256, (j + 1) * 256)
                total = jnp.zeros((64, 256), jnp.float32)
                for n in range(BANDS):
                    lhs = jnp.concatenate((left[0, n, rows, :], left[1, n, rows, :]), axis=0)
                    both = jnp.dot(lhs, right[n, :, cols], preferred_element_type=jnp.float32)
                    re = both[:64]
                    im = both[64:]
                    ci = col_inv[n, rows, :]
                    ci = jnp.concatenate((ci, ci), axis=1)
                    total += (re * re + im * im) * row_inv[n, 0:1, cols] * ci
                out_ref[s, :, cols] = total
        return carry

    lax.fori_loop(0, 8, tile, 0)


def pairs(core, x):
    shape = jax.ShapeDtypeStruct((8, 64, 1024), jnp.float32)
    return pl.pallas_call(
        pair_kernel,
        in_specs=[
            pl.BlockSpec(memory_space=pltpu.SMEM),
            pl.BlockSpec(memory_space=pltpu.VMEM),
        ],
        out_specs=[pl.BlockSpec(memory_space=pltpu.VMEM)] * 2,
        out_shape=[shape, shape],
        scratch_shapes=[
            pltpu.VMEM((BANDS, 256, 1024), jnp.bfloat16),
            pltpu.VMEM((2, BANDS, 1024, 256), jnp.bfloat16),
            pltpu.VMEM((BANDS, 8, 1024), jnp.float32),
            pltpu.VMEM((BANDS, 1024, 128), jnp.float32),
        ],
        compiler_params=pltpu.CompilerParams(vmem_limit_bytes=40 * 2**20),
    )(core, x)


def add_kernel(a_ref, b_ref, o_ref):
    for g in range(8):
        cols = slice(g * 128, (g + 1) * 128)
        o_ref[g] = a_ref[:, :, cols] + b_ref[:, :, cols]


def added(a, b):
    return pl.pallas_call(
        add_kernel,
        in_specs=[pl.BlockSpec(memory_space=pltpu.VMEM)] * 2,
        out_specs=pl.BlockSpec(memory_space=pltpu.VMEM),
        out_shape=jax.ShapeDtypeStruct((8, 8, 64, 128), jnp.float32),
    )(a, b)


def body(scale, coeffs):
    core = lax.axis_index("core")
    chan = lax.axis_index("chip") * 2 + core
    band = lax.axis_index("band")
    sent = turned(coeffs)
    mine = lax.all_to_all(sent, ("chip", "core"), 0, 0, tiled=True)
    own, other = pairs(core.astype(jnp.int32).reshape(1), mine)
    other = lax.ppermute(other, "core", [(0, 1), (1, 0)])
    blocks = added(own, other).reshape(64, 64, 128)
    blocks = lax.all_to_all(blocks, ("band", "chip"), 0, 0, tiled=True)
    total = jnp.sum(blocks, axis=0) * scale
    row = lax.broadcasted_iota(jnp.int32, (64, 128), 0) + chan * 64
    col = lax.broadcasted_iota(jnp.int32, (64, 128), 1) + band * 128
    return jnp.where(row == col, jnp.float32(0.0), total)


def solution(mesh):
    fine = Mesh(mesh.devices.reshape(8, 8, 2), ("band", "chip", "core"))
    scale = W * K / 512

    def whole(coeffs):
        return jax.shard_map(
            lambda x: body(scale, x),
            mesh=fine,
            in_specs=(P(None, None, ("chip", "core"), "band"),),
            out_specs=P(("chip", "core"), "band"),
            check_vma=False,
        )(coeffs)

    return whole
```

```python
import jax
import jax.numpy as jnp
from jax import lax
from jax.experimental import pallas as pl
from jax.experimental.pallas import tpu as pltpu
from jax.sharding import Mesh, PartitionSpec as P

K = 8
W = 16
EPS = 1e-06
CHUNKS = (8,)

LIMIT = 2.0**-11
SQUARE = 2.0**8
LINEAR = 2.0**26

WHOLE = pl.BlockSpec(memory_space=pltpu.VMEM)
SCALAR = pl.BlockSpec(memory_space=pltpu.SMEM)


def turn_kernel(core_ref, x_ref, *refs):
    outs = refs[: len(CHUNKS)]
    buffer, sems = refs[len(CHUNKS) :]
    core = core_ref[0]

    def fetch(k):
        return pltpu.make_async_copy(x_ref.at[:, k], buffer.at[k], sems.at[k])

    for k in range(K):
        fetch(k).start()

    def step(k, carry):
        fetch(k).wait()
        for t in range(8):
            lanes = slice(t * 128, (t + 1) * 128)
            first = buffer[k, core, :, lanes]
            second = buffer[k, 1 - core, :, lanes]
            both = jnp.concatenate((first, second), axis=0).T
            start = 0
            for o_ref, bands in zip(outs, CHUNKS):
                o_ref[t, k] = both[start : start + bands * W]
                start += bands * W
        return carry

    lax.fori_loop(0, K, step, 0)


def turned(core, coeffs):
    width, bins = coeffs.shape[2:]
    return pl.pallas_call(
        turn_kernel,
        in_specs=[SCALAR, pl.BlockSpec(memory_space=pltpu.HBM)],
        out_specs=[WHOLE] * len(CHUNKS),
        out_shape=[
            jax.ShapeDtypeStruct((8, K, bands * W, 128), jnp.bfloat16) for bands in CHUNKS
        ],
        scratch_shapes=[
            pltpu.VMEM((K, 2, width, bins), jnp.bfloat16),
            pltpu.SemaphoreType.DMA((K,)),
        ],
        compiler_params=pltpu.CompilerParams(vmem_limit_bytes=10 * 2**20),
    )(core, coeffs)


def left_kernel(core_ref, x_ref, left, col_inv):
    core = core_ref[0]
    bands = x_ref.shape[2] // W
    for n in range(bands):
        for s in range(8):
            block = jnp.concatenate(
                [x_ref[s, k, n * W : (n + 1) * W, :] for k in range(K)], axis=0
            )
            turned = block.T
            first = turned[:64]
            second = turned[64:]
            re = jnp.where(core == 0, first, second)
            im = jnp.where(core == 0, second, first)
            rows = slice(s * 64, (s + 1) * 64)
            left[0, n, rows, 0:128] = re
            left[0, n, rows, 128:256] = im
            left[1, n, rows, 0:128] = im
            left[1, n, rows, 128:256] = -re
            wide = block.astype(jnp.float32)
            halves = jnp.sum(wide * wide, axis=0, keepdims=True)
            power = halves + jnp.concatenate((halves[:, 64:], halves[:, :64]), axis=1)
            inv = 1.0 / (power + EPS)
            col_inv[n, rows, :] = jnp.broadcast_to(inv, (128, 128)).T[:64]


def lefts(core, x):
    bands = x.shape[2] // W
    return pl.pallas_call(
        left_kernel,
        in_specs=[SCALAR, WHOLE],
        out_specs=[WHOLE] * 2,
        out_shape=[
            jax.ShapeDtypeStruct((2, bands, 512, 256), jnp.bfloat16),
            jax.ShapeDtypeStruct((bands, 512, 128), jnp.float32),
        ],
        compiler_params=pltpu.CompilerParams(vmem_limit_bytes=16 * 2**20),
    )(core, x)


def pair_kernel(bands, first, last, core_ref, own_ref, other_ref, left, col_inv, *refs):
    refs = list(refs)
    before = None if first else refs.pop(0)
    o_ref, right, row_inv = refs
    core = core_ref[0]
    lane = lax.broadcasted_iota(jnp.int32, (bands * W, 128), 1)
    mine = (lane < 64) == (core == 0)
    for s in range(8):
        lanes = slice(s * 128, (s + 1) * 128)
        for k in range(K):
            own = own_ref[s, k]
            other = other_ref[s, k]
            re = jnp.where(mine, own, other)
            im = jnp.where(mine, other, own)
            im = jnp.concatenate((im[:, 64:], im[:, :64]), axis=1)
            for n in range(bands):
                right[n, k * W : (k + 1) * W, lanes] = re[n * W : (n + 1) * W]
                right[n, 128 + k * W : 128 + (k + 1) * W, lanes] = im[n * W : (n + 1) * W]

    for n in range(bands):
        for s in range(8):
            lanes = slice(s * 128, (s + 1) * 128)
            wide = right[n, :, lanes].astype(jnp.float32)
            power = jnp.sum(wide * wide, axis=0, keepdims=True) + EPS
            row_inv[n, :, lanes] = jnp.broadcast_to(1.0 / power, (8, 128))

    def tile(i, carry):
        rows = pl.ds(pl.multiple_of(i * 128, 128), 128)
        for j in range(4):
            cols = slice(j * 256, (j + 1) * 256)
            total = jnp.zeros((128, 256), jnp.float32)
            for n in range(bands):
                lhs = jnp.concatenate((left[0, n, rows, :], left[1, n, rows, :]), axis=0)
                both = jnp.dot(lhs, right[n, :, cols], preferred_element_type=jnp.float32)
                re = both[:128]
                im = both[128:]
                ci = col_inv[n, rows, :]
                ci = jnp.concatenate((ci, ci), axis=1)
                total += (re * re + im * im) * row_inv[n, 0:1, cols] * ci
            if before is not None:
                total += before[rows, cols]
            if last:
                coded = jnp.where(total >= LIMIT, total * total * SQUARE, total * -LINEAR)
                for h in range(2):
                    for g in range(2):
                        o_ref[2 * j + g, 2 * i + h] = coded[
                            h * 64 : (h + 1) * 64, g * 128 : (g + 1) * 128
                        ]
            else:
                o_ref[rows, cols] = total
        return carry

    lax.fori_loop(0, 4, tile, 0)


def pairs(core, own, other, left, col_inv, before, last):
    bands = own.shape[2] // W
    first = before is None
    if last:
        shape = jax.ShapeDtypeStruct((8, 8, 64, 128), jnp.float32)
    else:
        shape = jax.ShapeDtypeStruct((512, 1024), jnp.float32)
    args = (core, own, other, left, col_inv) + (() if first else (before,))
    return pl.pallas_call(
        lambda *refs: pair_kernel(bands, first, last, *refs),
        in_specs=[SCALAR] + [WHOLE] * (len(args) - 1),
        out_specs=WHOLE,
        out_shape=shape,
        scratch_shapes=[
            pltpu.VMEM((bands, 256, 1024), jnp.bfloat16),
            pltpu.VMEM((bands, 8, 1024), jnp.float32),
        ],
        compiler_params=pltpu.CompilerParams(vmem_limit_bytes=24 * 2**20),
    )(*args)


def body(scale, coeffs):
    core = lax.axis_index("core")
    chan = lax.axis_index("chip") * 2 + core
    band = lax.axis_index("band")
    core = core.astype(jnp.int32).reshape(1)
    total = None
    for c, sent in enumerate(turned(core, coeffs)):
        own = lax.all_to_all(sent, "chip", 0, 0, tiled=True)
        other = lax.ppermute(own, "core", [(0, 1), (1, 0)])
        left, col_inv = lefts(core, own)
        total = pairs(core, own, other, left, col_inv, total, c == len(CHUNKS) - 1)
    coded = total.reshape(64, 64, 128).astype(jnp.float16)
    coded = lax.all_to_all(coded, ("band", "chip"), 0, 0, tiled=True)
    coded = coded.astype(jnp.float32)
    value = jnp.where(coded < 0, coded * (-1 / LINEAR), jnp.sqrt(coded * (1 / SQUARE)))
    total = jnp.sum(value, axis=0) * scale
    row = lax.broadcasted_iota(jnp.int32, (64, 128), 0) + chan * 64
    col = lax.broadcasted_iota(jnp.int32, (64, 128), 1) + band * 128
    return jnp.where(row == col, jnp.float32(0.0), total)


def solution(mesh):
    fine = Mesh(mesh.devices.reshape(8, 8, 2), ("band", "chip", "core"))
    scale = W * K / 512

    def whole(coeffs):
        return jax.shard_map(
            lambda x: body(scale, x),
            mesh=fine,
            in_specs=(P(None, None, ("chip", "core"), "band"),),
            out_specs=P(("chip", "core"), "band"),
            check_vma=False,
        )(coeffs)

    return whole
```

```python
import jax
import jax.numpy as jnp
from jax import lax
from jax.experimental import pallas as pl
from jax.experimental.pallas import tpu as pltpu
from jax.sharding import Mesh, PartitionSpec as P

K = 8
W = 16
EPS = 1e-06
BANDS = 8

LIMIT = 2.0**-11
SQUARE = 2.0**8
LINEAR = 2.0**26

WHOLE = pl.BlockSpec(memory_space=pltpu.VMEM)
SCALAR = pl.BlockSpec(memory_space=pltpu.SMEM)


def swapped(x):
    return jnp.concatenate((x[:, 64:], x[:, :64]), axis=1)


def turn_kernel(core_ref, x_ref, o_ref):
    core = core_ref[0]

    def step(k, carry):
        for t in range(8):
            lanes = slice(t * 128, (t + 1) * 128)
            first = x_ref[core, k, :, lanes]
            second = x_ref[1 - core, k, :, lanes]
            o_ref[t, k] = jnp.concatenate((first, second), axis=0).T
        return carry

    lax.fori_loop(0, K, step, 0)


def turned(core, coeffs):
    return pl.pallas_call(
        turn_kernel,
        in_specs=[SCALAR, WHOLE],
        out_specs=WHOLE,
        out_shape=jax.ShapeDtypeStruct((8, K, 128, 128), jnp.bfloat16),
        compiler_params=pltpu.CompilerParams(vmem_limit_bytes=8 * 2**20),
    )(core, coeffs)


def arrange(side, x_ref, right, row_inv):
    low = lax.broadcasted_iota(jnp.int32, (128, 128), 1) < 64

    def step(m, carry):
        lanes = pl.ds(pl.multiple_of(m * 128, 128), 128)
        for k in range(K):
            a = x_ref[2 * m, k]
            b = x_ref[2 * m + 1, k]
            first = jnp.where(low, a, swapped(b))
            second = jnp.where(low, swapped(a), b)
            at_first = pl.ds(pl.multiple_of(side * 128 + k * W, W), W)
            at_second = pl.ds(pl.multiple_of((1 - side) * 128 + k * W, W), W)
            for n in range(BANDS):
                right[n, at_first, lanes] = first[n * W : (n + 1) * W]
                right[n, at_second, lanes] = second[n * W : (n + 1) * W]
        for n in range(BANDS):
            wide = right[n, :, lanes].astype(jnp.float32)
            power = jnp.sum(wide * wide, axis=0, keepdims=True) + EPS
            row_inv[n : n + 1, lanes] = 1.0 / power
        return carry

    lax.fori_loop(0, 4, step, 0)


def coherence(rows, cols, left, right, row_inv, col_inv):
    total = jnp.zeros((128, 256), jnp.float32)
    for n in range(BANDS):
        lhs = jnp.concatenate((left[0, n, rows, :], left[1, n, rows, :]), axis=0)
        both = jnp.dot(lhs, right[n, :, cols], preferred_element_type=jnp.float32)
        re = both[:128]
        im = both[128:]
        ci = col_inv[n, rows, :]
        ci = jnp.concatenate((ci, ci), axis=1)
        total += (re * re + im * im) * row_inv[n : n + 1, cols] * ci
    return total


def own_kernel(core_ref, x_ref, left, col_inv, o_ref, right, row_inv):
    arrange(core_ref[0], x_ref, right, row_inv)

    def turn(m, carry):
        lanes = pl.ds(pl.multiple_of(m * 128, 128), 128)
        columns = row_inv[:, lanes].T
        for n in range(BANDS):
            block = right[n, :, lanes].T
            left[0, n, lanes, :] = block
            left[1, n, lanes, 0:128] = block[:, 128:]
            left[1, n, lanes, 128:256] = -block[:, :128]
            col_inv[n, lanes, :] = jnp.broadcast_to(columns[:, n : n + 1], (128, 128))
        return carry

    lax.fori_loop(0, 4, turn, 0)

    def tile(i, carry):
        rows = pl.ds(pl.multiple_of(i * 128, 128), 128)
        for j in range(2):
            cols = slice(j * 256, (j + 1) * 256)
            o_ref[rows, cols] = coherence(rows, cols, left, right, row_inv, col_inv)
        return carry

    lax.fori_loop(0, 4, tile, 0)


ARRANGED = [
    pltpu.VMEM((BANDS, 256, 512), jnp.bfloat16),
    pltpu.VMEM((BANDS, 512), jnp.float32),
]


def own_pairs(core, x):
    return pl.pallas_call(
        own_kernel,
        in_specs=[SCALAR, WHOLE],
        out_specs=[WHOLE] * 3,
        out_shape=[
            jax.ShapeDtypeStruct((2, BANDS, 512, 256), jnp.bfloat16),
            jax.ShapeDtypeStruct((BANDS, 512, 128), jnp.float32),
            jax.ShapeDtypeStruct((512, 512), jnp.float32),
        ],
        scratch_shapes=ARRANGED,
        compiler_params=pltpu.CompilerParams(vmem_limit_bytes=16 * 2**20),
    )(core, x)


def other_kernel(core_ref, x_ref, left, col_inv, own_ref, o_ref, right, row_inv):
    arrange(1 - core_ref[0], x_ref, right, row_inv)
    first_core = core_ref[0] == 0
    low = lax.broadcasted_iota(jnp.int32, (128, 128), 1) < 64

    def tile(i, carry):
        rows = pl.ds(pl.multiple_of(i * 128, 128), 128)
        for j in range(2):
            cols = slice(j * 256, (j + 1) * 256)
            total = coherence(rows, cols, left, right, row_inv, col_inv)
            for half in range(2):
                m = 2 * j + half
                own = own_ref[rows, m * 128 : (m + 1) * 128]
                other = total[:, half * 128 : (half + 1) * 128]
                zero = jnp.where(first_core, own, other)
                one = jnp.where(first_core, other, own)
                for g in range(2):
                    if g == 0:
                        sums = jnp.where(low, zero, swapped(one))
                    else:
                        sums = jnp.where(low, swapped(zero), one)
                    coded = jnp.where(sums >= LIMIT, sums * sums * SQUARE, sums * -LINEAR)
                    for h in range(2):
                        o_ref[2 * m + g, 2 * i + h] = coded[h * 64 : (h + 1) * 64]
        return carry

    lax.fori_loop(0, 4, tile, 0)


def other_pairs(core, x, left, col_inv, own):
    return pl.pallas_call(
        other_kernel,
        in_specs=[SCALAR] + [WHOLE] * 4,
        out_specs=WHOLE,
        out_shape=jax.ShapeDtypeStruct((8, 8, 64, 128), jnp.float32),
        scratch_shapes=ARRANGED,
        compiler_params=pltpu.CompilerParams(vmem_limit_bytes=16 * 2**20),
    )(core, x, left, col_inv, own)


def body(scale, coeffs):
    core = lax.axis_index("core")
    chan = lax.axis_index("chip") * 2 + core
    band = lax.axis_index("band")
    side = core.astype(jnp.int32).reshape(1)
    own = lax.all_to_all(turned(side, coeffs), "chip", 0, 0, tiled=True)
    other = lax.ppermute(own, "core", [(0, 1), (1, 0)])
    left, col_inv, sums = own_pairs(side, own)
    coded = other_pairs(side, other, left, col_inv, sums)
    coded = coded.reshape(64, 64, 128).astype(jnp.float16)
    coded = lax.all_to_all(coded, ("band", "chip"), 0, 0, tiled=True).astype(jnp.float32)
    value = jnp.where(coded < 0, coded * (-1 / LINEAR), jnp.sqrt(coded * (1 / SQUARE)))
    row = lax.broadcasted_iota(jnp.int32, (64, 64, 128), 1) + chan * 64
    col = lax.broadcasted_iota(jnp.int32, (64, 64, 128), 2) + band * 128
    return jnp.sum(jnp.where(row == col, jnp.float32(0.0), value * scale), axis=0)


def solution(mesh):
    fine = Mesh(mesh.devices.reshape(8, 8, 2), ("band", "chip", "core"))
    scale = W * K / 512

    def whole(coeffs):
        return jax.shard_map(
            lambda x: body(scale, x),
            mesh=fine,
            in_specs=(P(None, None, ("chip", "core"), "band"),),
            out_specs=P(("chip", "core"), "band"),
            check_vma=False,
        )(coeffs)

    return whole
```

```python
import jax
import jax.numpy as jnp
from jax import lax
from jax.experimental import pallas as pl
from jax.experimental.pallas import tpu as pltpu
from jax.sharding import Mesh, PartitionSpec as P

K = 8
W = 16
EPS = 1e-06
BANDS = 8

LIMIT = 2.0**-11
SQUARE = 2.0**8
LINEAR = 2.0**26

WHOLE = pl.BlockSpec(memory_space=pltpu.VMEM)
SCALAR = pl.BlockSpec(memory_space=pltpu.SMEM)


def swapped(x):
    return jnp.concatenate((x[:, 64:], x[:, :64]), axis=1)


def turn_kernel(core_ref, x_hbm, o_ref, x_ref, sems):
    core = core_ref[0]

    def fetch(k):
        return pltpu.make_async_copy(x_hbm.at[:, k], x_ref.at[:, k], sems.at[k])

    for k in range(K):
        fetch(k).start()

    def step(k, carry):
        fetch(k).wait()
        for t in range(8):
            lanes = slice(t * 128, (t + 1) * 128)
            first = x_ref[core, k, :, lanes]
            second = x_ref[1 - core, k, :, lanes]
            o_ref[t, k] = jnp.concatenate((first, second), axis=0).T
        return carry

    lax.fori_loop(0, K, step, 0)


def turned(core, coeffs):
    return pl.pallas_call(
        turn_kernel,
        in_specs=[SCALAR, pl.BlockSpec(memory_space=pltpu.HBM)],
        out_specs=WHOLE,
        out_shape=jax.ShapeDtypeStruct((8, K, 128, 128), jnp.bfloat16),
        scratch_shapes=[
            pltpu.VMEM(coeffs.shape, jnp.bfloat16),
            pltpu.SemaphoreType.DMA((K,)),
        ],
        compiler_params=pltpu.CompilerParams(vmem_limit_bytes=8 * 2**20),
    )(core, pltpu.with_memory_space_constraint(coeffs, pltpu.HBM))


def arrange(side, x_ref, right, row_inv):
    low = lax.broadcasted_iota(jnp.int32, (128, 128), 1) < 64

    def step(m, carry):
        power = [jnp.zeros((8, 128), jnp.float32)] * BANDS
        for k in range(K):
            a = x_ref[2 * m, k]
            b = x_ref[2 * m + 1, k]
            for part, block in (
                (side, jnp.where(low, a, swapped(b))),
                (1 - side, jnp.where(low, swapped(a), b)),
            ):
                for n in range(BANDS):
                    rows = block[n * W : (n + 1) * W]
                    right[n, m, part * K + k] = rows
                    wide = rows.astype(jnp.float32)
                    wide = wide * wide
                    power[n] += wide[:8] + wide[8:]
        for n in range(BANDS):
            total = jnp.sum(power[n], axis=0, keepdims=True) + EPS
            row_inv[m, n : n + 1, :] = 1.0 / total
        return carry

    lax.fori_loop(0, 4, step, 0)


def coherence(rows, j, left, right, row_inv, col_inv):
    total = jnp.zeros((128, 256), jnp.float32)
    for n in range(BANDS):
        re = left[0, n, rows, :]
        im = left[1, n, rows, :]
        for_re = jnp.concatenate((re, im), axis=1)
        for_im = jnp.concatenate((im, left[2, n, rows, :]), axis=1)
        lhs = jnp.concatenate((for_re, for_im), axis=0)
        rhs = jnp.concatenate(
            (right[n, 2 * j].reshape(256, 128), right[n, 2 * j + 1].reshape(256, 128)), axis=1
        )
        both = jnp.dot(lhs, rhs, preferred_element_type=jnp.float32)
        re = both[:128]
        im = both[128:]
        ri = jnp.concatenate((row_inv[2 * j, n : n + 1, :], row_inv[2 * j + 1, n : n + 1, :]), axis=1)
        ci = col_inv[n, rows, :]
        ci = jnp.concatenate((ci, ci), axis=1)
        total += (re * re + im * im) * ri * ci
    return total


def own_kernel(core_ref, x_ref, left, col_inv, o_ref, right, row_inv):
    arrange(core_ref[0], x_ref, right, row_inv)

    def tile(i, carry):
        rows = pl.ds(pl.multiple_of(i * 128, 128), 128)
        columns = row_inv[i].T
        for n in range(BANDS):
            block = right[n, i].reshape(256, 128).T
            left[0, n, rows, :] = block[:, :128]
            left[1, n, rows, :] = block[:, 128:]
            left[2, n, rows, :] = -block[:, :128]
            col_inv[n, rows, :] = jnp.broadcast_to(columns[:, n : n + 1], (128, 128))
        row = lax.broadcasted_iota(jnp.int32, (128, 256), 0) + i * 128
        col = lax.broadcasted_iota(jnp.int32, (128, 256), 1)
        for j in range(2):
            cols = slice(j * 256, (j + 1) * 256)
            total = coherence(rows, j, left, right, row_inv, col_inv)
            o_ref[rows, cols] = jnp.where(row == col + j * 256, 0.0, total)
        return carry

    lax.fori_loop(0, 4, tile, 0)


ARRANGED = [
    pltpu.VMEM((BANDS, 4, 2 * K, W, 128), jnp.bfloat16),
    pltpu.VMEM((4, BANDS, 128), jnp.float32),
]


def own_pairs(core, x):
    return pl.pallas_call(
        own_kernel,
        in_specs=[SCALAR, WHOLE],
        out_specs=[WHOLE] * 3,
        out_shape=[
            jax.ShapeDtypeStruct((3, BANDS, 512, 128), jnp.bfloat16),
            jax.ShapeDtypeStruct((BANDS, 512, 128), jnp.float32),
            jax.ShapeDtypeStruct((512, 512), jnp.float32),
        ],
        scratch_shapes=ARRANGED,
        compiler_params=pltpu.CompilerParams(vmem_limit_bytes=16 * 2**20),
    )(core, x)


def other_kernel(core_ref, x_ref, left, col_inv, own_ref, o_ref, right, row_inv):
    arrange(1 - core_ref[0], x_ref, right, row_inv)
    first_core = core_ref[0] == 0
    low = lax.broadcasted_iota(jnp.int32, (128, 128), 1) < 64

    def tile(i, carry):
        rows = pl.ds(pl.multiple_of(i * 128, 128), 128)
        for j in range(2):
            total = coherence(rows, j, left, right, row_inv, col_inv)
            for half in range(2):
                m = 2 * j + half
                own = own_ref[rows, m * 128 : (m + 1) * 128]
                other = total[:, half * 128 : (half + 1) * 128]
                zero = jnp.where(first_core, own, other)
                one = jnp.where(first_core, other, own)
                for g in range(2):
                    if g == 0:
                        sums = jnp.where(low, zero, swapped(one))
                    else:
                        sums = jnp.where(low, swapped(zero), one)
                    coded = jnp.where(sums >= LIMIT, sums * sums * SQUARE, sums * -LINEAR)
                    for h in range(2):
                        o_ref[2 * i + h, 2 * m + g] = coded[h * 64 : (h + 1) * 64]
        return carry

    lax.fori_loop(0, 4, tile, 0)


def other_pairs(core, x, left, col_inv, own):
    return pl.pallas_call(
        other_kernel,
        in_specs=[SCALAR] + [WHOLE] * 4,
        out_specs=WHOLE,
        out_shape=jax.ShapeDtypeStruct((8, 8, 64, 128), jnp.float32),
        scratch_shapes=ARRANGED,
        compiler_params=pltpu.CompilerParams(vmem_limit_bytes=16 * 2**20),
    )(core, x, left, col_inv, own)


def body(scale, coeffs):
    core = lax.axis_index("core")
    side = core.astype(jnp.int32).reshape(1)
    own = lax.all_to_all(turned(side, coeffs), "chip", 0, 0, tiled=True)
    other = lax.ppermute(own, "core", [(0, 1), (1, 0)])
    left, col_inv, sums = own_pairs(side, own)
    coded = other_pairs(side, other, left, col_inv, sums)
    coded = coded.reshape(64, 64, 128).astype(jnp.float16)
    coded = lax.all_to_all(coded, ("chip", "band"), 0, 0, tiled=True).astype(jnp.float32)
    square = coded * lax.rsqrt(coded) * (scale / SQUARE**0.5)
    return jnp.sum(jnp.where(coded > 0, square, coded * (-scale / LINEAR)), axis=0)


def solution(mesh):
    fine = Mesh(mesh.devices.reshape(8, 8, 2), ("band", "chip", "core"))
    scale = W * K / 512

    def whole(coeffs):
        return jax.shard_map(
            lambda x: body(scale, x),
            mesh=fine,
            in_specs=(P(None, None, ("chip", "core"), "band"),),
            out_specs=P(("chip", "core"), "band"),
            check_vma=False,
        )(coeffs)

    return whole
```

```python
import jax
import jax.numpy as jnp
from jax import lax
from jax.experimental import pallas as pl
from jax.experimental.pallas import tpu as pltpu
from jax.sharding import Mesh, PartitionSpec as P


K = 8
W = 16
EPS = 1e-06
BANDS = 8

STEPS = ((0, 0), (0, 1), (0, 3), (0, 2), (1, 0), (1, 1), (1, 3), (1, 2))

LIMIT = 2.0**-11
SQUARE = 2.0**8
LINEAR = 2.0**26

WHOLE = pl.BlockSpec(memory_space=pltpu.VMEM)
SCALAR = pl.BlockSpec(memory_space=pltpu.SMEM)
PIECE = (K, BANDS * W, 128)
ARRANGED = (BANDS, 2, 2 * K + 1, W, 128)


def chip_at(chip, step, sign):
    half = (chip >> 2) ^ step[0]
    return (half << 2) + ((chip + sign * step[1]) & 3)


def swapped(x):
    return jnp.concatenate((x[:, 64:], x[:, :64]), axis=1)


def call(kernel, mib, out, scratch=(), products=0):
    many = isinstance(out, list)

    def run(place, *args, first=WHOLE):
        return pl.pallas_call(
            kernel,
            in_specs=[SCALAR, first] + [WHOLE] * (len(args) - 1),
            out_specs=[WHOLE] * len(out) if many else WHOLE,
            out_shape=out,
            scratch_shapes=list(scratch),
            cost_estimate=pl.CostEstimate(
                flops=products * BANDS * 2 * 256**3, bytes_accessed=2**20, transcendentals=0
            ),
            compiler_params=pltpu.CompilerParams(vmem_limit_bytes=mib * 2**20),
        )(place, *args)

    return run


def turn_kernel(place, x_hbm, *refs):
    outs = refs[: len(STEPS)]
    x_ref, sems = refs[len(STEPS) :]
    core = place[0]
    chip = place[1]

    def fetch(k):
        return pltpu.make_async_copy(x_hbm.at[:, k], x_ref.at[:, k], sems.at[k])

    for k in range(K):
        fetch(k).start()

    def step(k, carry):
        fetch(k).wait()
        for o_ref, go in zip(outs, STEPS):
            lanes = pl.ds(pl.multiple_of(chip_at(chip, go, 1) * 128, 128), 128)
            first = x_ref[core, k, :, lanes]
            second = x_ref[1 - core, k, :, lanes]
            o_ref[k] = jnp.concatenate((first, second), axis=0).T
        return carry

    lax.fori_loop(0, K, step, 0)


def turned(place, coeffs):
    piece = jax.ShapeDtypeStruct(PIECE, jnp.bfloat16)
    run = call(
        turn_kernel,
        8,
        [piece] * len(STEPS),
        (pltpu.VMEM(coeffs.shape, jnp.bfloat16), pltpu.SemaphoreType.DMA((K,))),
    )
    coeffs = pltpu.with_memory_space_constraint(coeffs, pltpu.HBM)
    return run(place, coeffs, first=pl.BlockSpec(memory_space=pltpu.HBM))


def arrange_kernel(place, x0, x1, x2, x3, right):
    side = place[0]
    low = lax.broadcasted_iota(jnp.int32, (128, 128), 1) < 64
    row = lax.broadcasted_iota(jnp.int32, (W, 128), 0)
    for m, (a_ref, b_ref) in enumerate(((x0, x1), (x2, x3))):

        def step(k, power):
            power = list(power)
            a = a_ref[k]
            b = b_ref[k]
            for part, block in (
                (side, jnp.where(low, a, swapped(b))),
                (1 - side, jnp.where(low, swapped(a), b)),
            ):
                for n in range(BANDS):
                    rows = block[n * W : (n + 1) * W]
                    right[n, m, part * K + k] = rows
                    wide = rows.astype(jnp.float32)
                    wide = wide * wide
                    power[n] += wide[:8] + wide[8:]
            return tuple(power)

        power = (jnp.zeros((8, 128), jnp.float32),) * BANDS
        for k in range(K):
            power = step(k, power)
        for n in range(BANDS):
            inv = 1.0 / (jnp.sum(power[n], axis=0, keepdims=True) + EPS)
            high = inv.astype(jnp.bfloat16).astype(jnp.float32)
            middle = (inv - high).astype(jnp.bfloat16).astype(jnp.float32)
            rest = inv - high - middle
            parts = jnp.where(row == 0, high, jnp.where(row == 1, middle, jnp.where(row == 2, rest, 0.0)))
            right[n, m, 2 * K] = parts.astype(jnp.bfloat16)


arranged = call(arrange_kernel, 8, jax.ShapeDtypeStruct(ARRANGED, jnp.bfloat16), products=1)


def inverse(right, n, m):
    parts = right[n, m, 2 * K].astype(jnp.float32)
    return jnp.sum(parts, axis=0, keepdims=True)


def columns(right, n, m):
    return right[n, m, 0 : 2 * K].reshape(256, 128)


def turn_left(i, right, left, col_inv):
    rows = pl.ds(pl.multiple_of(i * 128, 128), 128)
    inv = jnp.concatenate([inverse(right, n, i) for n in range(BANDS)], axis=0).T
    for n in range(BANDS):
        block = columns(right, n, i).T
        left[0, n, rows, :] = block[:, :128]
        left[1, n, rows, :] = block[:, 128:]
        left[2, n, rows, :] = -block[:, :128]
        col_inv[n, rows, :] = jnp.broadcast_to(inv[:, n : n + 1], (128, 128))


def coherence(i, left, col_inv, right):
    rows = pl.ds(pl.multiple_of(i * 128, 128), 128)
    total = jnp.zeros((128, 256), jnp.float32)
    for n in range(BANDS):
        re = left[0, n, rows, :]
        im = left[1, n, rows, :]
        for_re = jnp.concatenate((re, im), axis=1)
        for_im = jnp.concatenate((im, left[2, n, rows, :]), axis=1)
        lhs = jnp.concatenate((for_re, for_im), axis=0)
        rhs = jnp.concatenate((columns(right, n, 0), columns(right, n, 1)), axis=1)
        both = jnp.dot(lhs, rhs, preferred_element_type=jnp.float32)
        re = both[:128]
        im = both[128:]
        ri = jnp.concatenate((inverse(right, n, 0), inverse(right, n, 1)), axis=1)
        ci = col_inv[n, rows, :]
        ci = jnp.concatenate((ci, ci), axis=1)
        total += (re * re + im * im) * ri * ci
    return total


def no_diagonal(i, total):
    row = lax.broadcasted_iota(jnp.int32, (128, 256), 0) + i * 128
    col = lax.broadcasted_iota(jnp.int32, (128, 256), 1)
    return jnp.where(row == col, 0.0, total)


LEFT = jax.ShapeDtypeStruct((3, BANDS, 256, 128), jnp.bfloat16)
COL_INV = jax.ShapeDtypeStruct((BANDS, 256, 128), jnp.float32)
BLOCK = jax.ShapeDtypeStruct((256, 256), jnp.float32)


def near_own_kernel(place, right, left, col_inv, o_ref):
    def tile(i, carry):
        rows = pl.ds(pl.multiple_of(i * 128, 128), 128)
        turn_left(i, right, left, col_inv)
        o_ref[rows, :] = no_diagonal(i, coherence(i, left, col_inv, right))
        return carry

    lax.fori_loop(0, 2, tile, 0)


def near_other_kernel(place, right, left, col_inv, o_ref):
    def tile(i, carry):
        rows = pl.ds(pl.multiple_of(i * 128, 128), 128)
        o_ref[rows, :] = coherence(i, left, col_inv, right)
        return carry

    lax.fori_loop(0, 2, tile, 0)


def far_own_kernel(place, right0, right1, left1, col_inv1, o10, o11):
    def tile(i, carry):
        rows = pl.ds(pl.multiple_of(i * 128, 128), 128)
        turn_left(i, right1, left1, col_inv1)
        o10[rows, :] = coherence(i, left1, col_inv1, right0)
        o11[rows, :] = no_diagonal(i, coherence(i, left1, col_inv1, right1))
        return carry

    lax.fori_loop(0, 2, tile, 0)


def far_other_kernel(
    place, right0, right1, left0, col_inv0, left1, col_inv1, a00, a10, a11, b00, o_ref
):
    first_core = place[0] == 0
    chip = place[1]
    low = lax.broadcasted_iota(jnp.int32, (128, 128), 1) < 64

    def put(i, a, b, own_ref, total):
        rows = pl.ds(pl.multiple_of(i * 128, 128), 128)
        for m in range(2):
            lanes = slice(m * 128, (m + 1) * 128)
            own = own_ref[lanes, rows].T if a < b else own_ref[rows, lanes]
            other = total[:, lanes]
            zero = jnp.where(first_core, own, other)
            one = jnp.where(first_core, other, own)
            for g in range(2):
                if g == 0:
                    sums = jnp.where(low, zero, swapped(one))
                else:
                    sums = jnp.where(low, swapped(zero), one)
                coded = jnp.where(sums >= LIMIT, sums * sums * SQUARE, sums * -LINEAR)
                to = chip_at(chip, STEPS[4 * b + 2 * m + g], -1)
                for h in range(2):
                    even = chip_at(chip, STEPS[4 * a + h], -1)
                    odd = chip_at(chip, STEPS[4 * a + 2 + h], -1)
                    o_ref[jnp.where(i == 0, even, odd), to] = coded[h * 64 : (h + 1) * 64]

    def tile(i, carry):
        rows = pl.ds(pl.multiple_of(i * 128, 128), 128)
        put(i, 0, 0, a00, b00[rows, :])
        put(i, 0, 1, a10, coherence(i, left0, col_inv0, right1))
        put(i, 1, 0, a10, coherence(i, left1, col_inv1, right0))
        put(i, 1, 1, a11, coherence(i, left1, col_inv1, right1))
        return carry

    lax.fori_loop(0, 2, tile, 0)


near_own = call(near_own_kernel, 8, [LEFT, COL_INV, BLOCK], products=2)
near_other = call(near_other_kernel, 8, BLOCK, products=2)
far_own = call(far_own_kernel, 8, [LEFT, COL_INV, BLOCK, BLOCK], products=4)
far_other = call(
    far_other_kernel, 8, jax.ShapeDtypeStruct((8, 8, 64, 128), jnp.float32), products=6
)


def body(scale, coeffs):
    core = lax.axis_index("core")
    chip = lax.axis_index("chip")
    place = jnp.stack((core, chip)).astype(jnp.int32)
    pieces = list(turned(place, coeffs))
    for p in range(1, len(STEPS)):
        pairs = [(c, chip_at(c, STEPS[p], 1)) for c in range(8)]
        pieces[p] = lax.ppermute(pieces[p], "chip", pairs)
    swap = [(0, 1), (1, 0)]
    own0 = arranged(place, *pieces[:4])
    other0 = lax.ppermute(own0, "core", swap)
    left0, col_inv0, a00 = near_own(place, own0)
    b00 = near_other(place, other0, left0, col_inv0)
    own1 = arranged(place, *pieces[4:])
    other1 = lax.ppermute(own1, "core", swap)
    left1, col_inv1, a10, a11 = far_own(place, own0, own1)
    coded = far_other(
        place, other0, other1, left0, col_inv0, left1, col_inv1, a00, a10, a11, b00
    )
    coded = coded.reshape(64, 64, 128).astype(jnp.float16)
    coded = lax.all_to_all(coded, ("chip", "band"), 0, 0, tiled=True).astype(jnp.float32)
    square = coded * lax.rsqrt(coded) * (scale / SQUARE**0.5)
    return jnp.sum(jnp.where(coded > 0, square, coded * (-scale / LINEAR)), axis=0)


def solution(mesh):
    fine = Mesh(mesh.devices.reshape(8, 8, 2), ("band", "chip", "core"))
    scale = W * K / 512

    def step(coeffs):
        return body(scale, coeffs)

    return jax.shard_map(
        step,
        mesh=fine,
        in_specs=(P(None, None, ("chip", "core"), "band"),),
        out_specs=P(("chip", "core"), "band"),
        check_vma=False,
    )
```

```python
import jax
import jax.numpy as jnp
from jax import lax
from jax.experimental import pallas as pl
from jax.experimental.pallas import tpu as pltpu
from jax.sharding import Mesh, PartitionSpec as P


K = 8
W = 16
EPS = 1e-06
BANDS = 8

STEPS = ((0, 0), (0, 1), (0, 3), (0, 2), (1, 0), (1, 1), (1, 3), (1, 2))
ORDER = (1, 2, 4, 5, 3, 6, 7)
SPLIT = 3

LIMIT = 2.0**-11
SQUARE = 2.0**8
LINEAR = 2.0**26

WHOLE = pl.BlockSpec(memory_space=pltpu.VMEM)
SCALAR = pl.BlockSpec(memory_space=pltpu.SMEM)
PIECE = (K, BANDS * W, 128)
ARRANGED = (BANDS, 2, 2 * K + 1, W, 128)


def chip_at(chip, step, sign):
    half = (chip >> 2) ^ step[0]
    return (half << 2) + ((chip + sign * step[1]) & 3)


def swapped(x):
    return jnp.concatenate((x[:, 64:], x[:, :64]), axis=1)


def call(kernel, mib, out, scratch=(), products=0):
    many = isinstance(out, list)

    def run(place, *args, first=WHOLE):
        return pl.pallas_call(
            kernel,
            in_specs=[SCALAR, first] + [WHOLE] * (len(args) - 1),
            out_specs=[WHOLE] * len(out) if many else WHOLE,
            out_shape=out,
            scratch_shapes=list(scratch),
            cost_estimate=pl.CostEstimate(
                flops=products * BANDS * 2 * 256**3, bytes_accessed=2**20, transcendentals=0
            ),
            compiler_params=pltpu.CompilerParams(vmem_limit_bytes=mib * 2**20),
        )(place, *args)

    return run


def turn_kernel(steps, place, x_hbm, *refs):
    outs = refs[: len(steps)]
    x_ref, sems = refs[len(steps) :]
    core = place[0]
    chip = place[1]

    def fetch(p):
        lanes = pl.ds(pl.multiple_of(chip_at(chip, steps[p], 1) * 128, 128), 128)
        return pltpu.make_async_copy(x_hbm.at[:, :, :, lanes], x_ref.at[p], sems.at[p])

    for p in range(len(steps)):
        fetch(p).start()
    for p in range(len(steps)):
        fetch(p).wait()

    def step(h, carry):
        for k in range(K // 2):
            for p, o_ref in enumerate(outs):
                first = x_ref[p, core, h * (K // 2) + k]
                second = x_ref[p, 1 - core, h * (K // 2) + k]
                o_ref[h * (K // 2) + k] = jnp.concatenate((first, second), axis=0).T
        return carry

    lax.fori_loop(0, 2, step, 0)


def turned(place, coeffs, steps):
    run = call(
        lambda *refs: turn_kernel(steps, *refs),
        8,
        [jax.ShapeDtypeStruct(PIECE, jnp.bfloat16)] * len(steps),
        (
            pltpu.VMEM((len(steps), 2, K, coeffs.shape[2], 128), jnp.bfloat16),
            pltpu.SemaphoreType.DMA((len(steps),)),
        ),
    )
    return run(place, coeffs, first=pl.BlockSpec(memory_space=pltpu.HBM))


def arrange_kernel(place, x0, x1, x2, x3, right):
    side = place[0]
    low = lax.broadcasted_iota(jnp.int32, (128, 128), 1) < 64
    row = lax.broadcasted_iota(jnp.int32, (W, 128), 0)
    for m, (a_ref, b_ref) in enumerate(((x0, x1), (x2, x3))):

        def step(k, power):
            power = list(power)
            a = a_ref[k]
            b = b_ref[k]
            for part, block in (
                (side, jnp.where(low, a, swapped(b))),
                (1 - side, jnp.where(low, swapped(a), b)),
            ):
                for n in range(BANDS):
                    rows = block[n * W : (n + 1) * W]
                    right[n, m, part * K + k] = rows
                    wide = rows.astype(jnp.float32)
                    wide = wide * wide
                    power[n] += wide[:8] + wide[8:]
            return tuple(power)

        power = (jnp.zeros((8, 128), jnp.float32),) * BANDS
        for k in range(K):
            power = step(k, power)
        for n in range(BANDS):
            inv = 1.0 / (jnp.sum(power[n], axis=0, keepdims=True) + EPS)
            high = inv.astype(jnp.bfloat16).astype(jnp.float32)
            middle = (inv - high).astype(jnp.bfloat16).astype(jnp.float32)
            rest = inv - high - middle
            parts = jnp.where(row == 0, high, jnp.where(row == 1, middle, jnp.where(row == 2, rest, 0.0)))
            right[n, m, 2 * K] = parts.astype(jnp.bfloat16)


arranged = call(arrange_kernel, 8, jax.ShapeDtypeStruct(ARRANGED, jnp.bfloat16), products=1)


def inverse(right, n, m):
    parts = right[n, m, 2 * K].astype(jnp.float32)
    return jnp.sum(parts, axis=0, keepdims=True)


def columns(right, n, m):
    return right[n, m, 0 : 2 * K].reshape(256, 128)


def turn_left(i, right, left, col_inv):
    rows = pl.ds(pl.multiple_of(i * 128, 128), 128)
    inv = jnp.concatenate([inverse(right, n, i) for n in range(BANDS)], axis=0).T
    for n in range(BANDS):
        block = columns(right, n, i).T
        left[0, n, rows, :] = block[:, :128]
        left[1, n, rows, :] = block[:, 128:]
        left[2, n, rows, :] = -block[:, :128]
        col_inv[n, rows, :] = jnp.broadcast_to(inv[:, n : n + 1], (128, 128))


def coherence(i, left, col_inv, right):
    rows = pl.ds(pl.multiple_of(i * 128, 128), 128)
    total = jnp.zeros((128, 256), jnp.float32)
    for n in range(BANDS):
        re = left[0, n, rows, :]
        im = left[1, n, rows, :]
        for_re = jnp.concatenate((re, im), axis=1)
        for_im = jnp.concatenate((im, left[2, n, rows, :]), axis=1)
        lhs = jnp.concatenate((for_re, for_im), axis=0)
        rhs = jnp.concatenate((columns(right, n, 0), columns(right, n, 1)), axis=1)
        both = jnp.dot(lhs, rhs, preferred_element_type=jnp.float32)
        re = both[:128]
        im = both[128:]
        ri = jnp.concatenate((inverse(right, n, 0), inverse(right, n, 1)), axis=1)
        ci = col_inv[n, rows, :]
        ci = jnp.concatenate((ci, ci), axis=1)
        total += (re * re + im * im) * ri * ci
    return total


def no_diagonal(i, total):
    row = lax.broadcasted_iota(jnp.int32, (128, 256), 0) + i * 128
    col = lax.broadcasted_iota(jnp.int32, (128, 256), 1)
    return jnp.where(row == col, 0.0, total)


LEFT = jax.ShapeDtypeStruct((3, BANDS, 256, 128), jnp.bfloat16)
COL_INV = jax.ShapeDtypeStruct((BANDS, 256, 128), jnp.float32)
BLOCK = jax.ShapeDtypeStruct((256, 256), jnp.float32)


def near_own_kernel(place, right, left, col_inv, o_ref):
    def tile(i, carry):
        rows = pl.ds(pl.multiple_of(i * 128, 128), 128)
        turn_left(i, right, left, col_inv)
        o_ref[rows, :] = no_diagonal(i, coherence(i, left, col_inv, right))
        return carry

    lax.fori_loop(0, 2, tile, 0)


def near_other_kernel(place, right, left, col_inv, o_ref):
    def tile(i, carry):
        rows = pl.ds(pl.multiple_of(i * 128, 128), 128)
        o_ref[rows, :] = coherence(i, left, col_inv, right)
        return carry

    lax.fori_loop(0, 2, tile, 0)


def far_own_kernel(place, right0, right1, left1, col_inv1, o10, o11):
    def tile(i, carry):
        rows = pl.ds(pl.multiple_of(i * 128, 128), 128)
        turn_left(i, right1, left1, col_inv1)
        o10[rows, :] = coherence(i, left1, col_inv1, right0)
        o11[rows, :] = no_diagonal(i, coherence(i, left1, col_inv1, right1))
        return carry

    lax.fori_loop(0, 2, tile, 0)


def far_other_kernel(
    place, right0, right1, left0, col_inv0, left1, col_inv1, a00, a10, a11, b00, o_ref
):
    first_core = place[0] == 0
    chip = place[1]
    low = lax.broadcasted_iota(jnp.int32, (128, 128), 1) < 64

    def put(i, a, b, own_ref, total):
        rows = pl.ds(pl.multiple_of(i * 128, 128), 128)
        for m in range(2):
            lanes = slice(m * 128, (m + 1) * 128)
            own = own_ref[lanes, rows].T if a < b else own_ref[rows, lanes]
            other = total[:, lanes]
            zero = jnp.where(first_core, own, other)
            one = jnp.where(first_core, other, own)
            for g in range(2):
                if g == 0:
                    sums = jnp.where(low, zero, swapped(one))
                else:
                    sums = jnp.where(low, swapped(zero), one)
                coded = jnp.where(sums >= LIMIT, sums * sums * SQUARE, sums * -LINEAR)
                to = chip_at(chip, STEPS[4 * b + 2 * m + g], -1)
                for h in range(2):
                    even = chip_at(chip, STEPS[4 * a + h], -1)
                    odd = chip_at(chip, STEPS[4 * a + 2 + h], -1)
                    o_ref[jnp.where(i == 0, even, odd), to] = coded[h * 64 : (h + 1) * 64]

    def tile(i, carry):
        rows = pl.ds(pl.multiple_of(i * 128, 128), 128)
        put(i, 0, 0, a00, b00[rows, :])
        put(i, 0, 1, a10, coherence(i, left0, col_inv0, right1))
        put(i, 1, 0, a10, coherence(i, left1, col_inv1, right0))
        put(i, 1, 1, a11, coherence(i, left1, col_inv1, right1))
        return carry

    lax.fori_loop(0, 2, tile, 0)


near_own = call(near_own_kernel, 8, [LEFT, COL_INV, BLOCK], products=2)
near_other = call(near_other_kernel, 8, BLOCK, products=2)
far_own = call(far_own_kernel, 8, [LEFT, COL_INV, BLOCK, BLOCK], products=4)
far_other = call(
    far_other_kernel, 8, jax.ShapeDtypeStruct((8, 8, 64, 128), jnp.float32), products=6
)


def body(scale, coeffs):
    core = lax.axis_index("core")
    chip = lax.axis_index("chip")
    place = jnp.stack((core, chip)).astype(jnp.int32)
    coeffs = pltpu.with_memory_space_constraint(coeffs, pltpu.HBM)
    pieces = [None] * len(STEPS)
    for some in (ORDER[:SPLIT], ORDER[SPLIT:] + (0,)):
        for p, piece in zip(some, turned(place, coeffs, [STEPS[p] for p in some])):
            pieces[p] = piece
    for p in range(1, len(STEPS)):
        pairs = [(c, chip_at(c, STEPS[p], 1)) for c in range(8)]
        pieces[p] = lax.ppermute(pieces[p], "chip", pairs)
    swap = [(0, 1), (1, 0)]
    own0 = arranged(place, *pieces[:4])
    other0 = lax.ppermute(own0, "core", swap)
    left0, col_inv0, a00 = near_own(place, own0)
    b00 = near_other(place, other0, left0, col_inv0)
    own1 = arranged(place, *pieces[4:])
    other1 = lax.ppermute(own1, "core", swap)
    left1, col_inv1, a10, a11 = far_own(place, own0, own1)
    coded = far_other(
        place, other0, other1, left0, col_inv0, left1, col_inv1, a00, a10, a11, b00
    )
    coded = coded.reshape(64, 64, 128).astype(jnp.float16)
    coded = lax.all_to_all(coded, ("chip", "band"), 0, 0, tiled=True).astype(jnp.float32)
    square = coded * lax.rsqrt(coded) * (scale / SQUARE**0.5)
    return jnp.sum(jnp.where(coded > 0, square, coded * (-scale / LINEAR)), axis=0)


def solution(mesh):
    fine = Mesh(mesh.devices.reshape(8, 8, 2), ("band", "chip", "core"))
    scale = W * K / 512

    def step(coeffs):
        return body(scale, coeffs)

    return jax.shard_map(
        step,
        mesh=fine,
        in_specs=(P(None, None, ("chip", "core"), "band"),),
        out_specs=P(("chip", "core"), "band"),
        check_vma=False,
    )
```

```python
import jax
import jax.numpy as jnp
from jax import lax
from jax.experimental import pallas as pl
from jax.experimental.pallas import tpu as pltpu
from jax.sharding import Mesh, PartitionSpec as P


K = 8
W = 16
EPS = 1e-06
BANDS = 8

STEPS = ((0, 0), (0, 1), (0, 3), (1, 0), (0, 2), (1, 1), (1, 3), (1, 2))
ORDER = (1, 2, 3, 5, 4, 6, 7)
SPLIT = 3

LIMIT = 2.0**-11
SQUARE = 2.0**8
LINEAR = 2.0**26

WHOLE = pl.BlockSpec(memory_space=pltpu.VMEM)
SCALAR = pl.BlockSpec(memory_space=pltpu.SMEM)
PIECE = (K, BANDS * W, 128)


def chip_at(chip, step, sign):
    half = (chip >> 2) ^ step[0]
    return (half << 2) + ((chip + sign * step[1]) & 3)


def swapped(x):
    return jnp.concatenate((x[:, 64:], x[:, :64]), axis=1)


def call(kernel, mib, out, scratch=(), products=0, aliases=None):
    many = isinstance(out, list)

    def run(place, *args, first=WHOLE):
        return pl.pallas_call(
            kernel,
            in_specs=[SCALAR, first] + [WHOLE] * (len(args) - 1),
            out_specs=[WHOLE] * len(out) if many else WHOLE,
            out_shape=out,
            scratch_shapes=list(scratch),
            input_output_aliases=aliases or {},
            cost_estimate=pl.CostEstimate(
                flops=products * BANDS * 2 * 256**3, bytes_accessed=2**20, transcendentals=0
            ),
            compiler_params=pltpu.CompilerParams(vmem_limit_bytes=mib * 2**20),
        )(place, *args)

    return run


def turn_kernel(steps, place, x_hbm, *refs):
    outs = refs[: len(steps)]
    x_ref, sems = refs[len(steps) :]
    core = place[0]
    chip = place[1]

    def fetch(p, k):
        lanes = pl.ds(pl.multiple_of(chip_at(chip, steps[p], 1) * 128, 128), 128)
        return pltpu.make_async_copy(x_hbm.at[:, k, :, lanes], x_ref.at[p, :, k], sems.at[p, k])

    for k in range(K):
        for p in range(len(steps)):
            fetch(p, k).start()

    def step(h, carry):
        for k in range(K // 2):
            for p in range(len(steps)):
                fetch(p, h * (K // 2) + k).wait()
        for k in range(K // 2):
            for p, o_ref in enumerate(outs):
                first = x_ref[p, core, h * (K // 2) + k]
                second = x_ref[p, 1 - core, h * (K // 2) + k]
                o_ref[h * (K // 2) + k] = jnp.concatenate((first, second), axis=0).T
        return carry

    lax.fori_loop(0, 2, step, 0)


def turned(place, coeffs, steps):
    run = call(
        lambda *refs: turn_kernel(steps, *refs),
        8,
        [jax.ShapeDtypeStruct(PIECE, jnp.bfloat16)] * len(steps),
        (
            pltpu.VMEM((len(steps), 2, K, coeffs.shape[2], 128), jnp.bfloat16),
            pltpu.SemaphoreType.DMA((len(steps), K)),
        ),
    )
    return run(place, coeffs, first=pl.BlockSpec(memory_space=pltpu.HBM))


def arrange_kernel(place, *refs):
    *pieces, right = refs
    side = place[0]
    low = lax.broadcasted_iota(jnp.int32, (128, 128), 1) < 64
    row = lax.broadcasted_iota(jnp.int32, (W, 128), 0)
    for m, (a_ref, b_ref) in enumerate(zip(pieces[::2], pieces[1::2])):

        def step(k, power):
            power = list(power)
            a = a_ref[k]
            b = b_ref[k]
            for part, block in (
                (side, jnp.where(low, a, swapped(b))),
                (1 - side, jnp.where(low, swapped(a), b)),
            ):
                for n in range(BANDS):
                    rows = block[n * W : (n + 1) * W]
                    right[n, m, part * K + k] = rows
                    wide = rows.astype(jnp.float32)
                    wide = wide * wide
                    power[n] += wide[:8] + wide[8:]
            return tuple(power)

        power = (jnp.zeros((8, 128), jnp.float32),) * BANDS
        for k in range(K):
            power = step(k, power)
        for n in range(BANDS):
            inv = 1.0 / (jnp.sum(power[n], axis=0, keepdims=True) + EPS)
            high = inv.astype(jnp.bfloat16).astype(jnp.float32)
            middle = (inv - high).astype(jnp.bfloat16).astype(jnp.float32)
            rest = inv - high - middle
            parts = jnp.where(row == 0, high, jnp.where(row == 1, middle, jnp.where(row == 2, rest, 0.0)))
            right[n, m, 2 * K] = parts.astype(jnp.bfloat16)


def arranged(place, *pieces):
    shape = (BANDS, len(pieces) // 2, 2 * K + 1, W, 128)
    return call(arrange_kernel, 8, jax.ShapeDtypeStruct(shape, jnp.bfloat16), products=1)(place, *pieces)


def inverse(right, n, m):
    parts = right[n, m, 2 * K].astype(jnp.float32)
    return jnp.sum(parts, axis=0, keepdims=True)


def columns(right, n, m):
    return right[n, m, 0 : 2 * K].reshape(256, 128)


def tile_rows(i):
    return pl.ds(i * 128 if isinstance(i, int) else pl.multiple_of(i * 128, 128), 128)


def turn_left(i, right, m, left, col_inv):
    rows = tile_rows(i)
    inv = jnp.concatenate([inverse(right, n, m) for n in range(BANDS)], axis=0).T
    for n in range(BANDS):
        block = columns(right, n, m).T
        left[0, n, rows, :] = block[:, :128]
        left[1, n, rows, :] = block[:, 128:]
        left[2, n, rows, :] = -block[:, :128]
        col_inv[n, rows, :] = jnp.broadcast_to(inv[:, n : n + 1], (128, 128))


def coherence(i, left, col_inv, cols):
    rows = tile_rows(i)
    total = jnp.zeros((128, 128 * len(cols)), jnp.float32)
    for n in range(BANDS):
        re = left[0, n, rows, :]
        im = left[1, n, rows, :]
        for_re = jnp.concatenate((re, im), axis=1)
        for_im = jnp.concatenate((im, left[2, n, rows, :]), axis=1)
        lhs = jnp.concatenate((for_re, for_im), axis=0)
        rhs = jnp.concatenate([columns(right, n, m) for right, m in cols], axis=1)
        both = jnp.dot(lhs, rhs, preferred_element_type=jnp.float32)
        re = both[:128]
        im = both[128:]
        ri = jnp.concatenate([inverse(right, n, m) for right, m in cols], axis=1)
        ci = jnp.concatenate([col_inv[n, rows, :]] * len(cols), axis=1)
        total += (re * re + im * im) * ri * ci
    return total


def no_diagonal(first, total):
    row = lax.broadcasted_iota(jnp.int32, total.shape, 0) + first
    col = lax.broadcasted_iota(jnp.int32, total.shape, 1)
    return jnp.where(row == col, 0.0, total)


def put(place, o_ref, i, b, own, other):
    first_core = place[0] == 0
    chip = place[1]
    low = lax.broadcasted_iota(jnp.int32, (128, 128), 1) < 64
    froms = []
    for h in range(2):
        at = chip_at(chip, STEPS[h], -1)
        for t in range(1, 4):
            at = jnp.where(i == t, chip_at(chip, STEPS[2 * t + h], -1), at)
        froms.append(at)
    for m in range(2):
        lanes = slice(m * 128, (m + 1) * 128)
        zero = jnp.where(first_core, own[:, lanes], other[:, lanes])
        one = jnp.where(first_core, other[:, lanes], own[:, lanes])
        for g in range(2):
            if g == 0:
                sums = jnp.where(low, zero, swapped(one))
            else:
                sums = jnp.where(low, swapped(zero), one)
            coded = jnp.where(sums >= LIMIT, sums * sums * SQUARE, sums * -LINEAR)
            to = chip_at(chip, STEPS[4 * b + 2 * m + g], -1)
            for h in range(2):
                o_ref[froms[h], to] = coded[h * 64 : (h + 1) * 64]


def both_of(right):
    return ((right, 0), (right, 1))


LEFT = jax.ShapeDtypeStruct((3, BANDS, 512, 128), jnp.bfloat16)
COL_INV = jax.ShapeDtypeStruct((BANDS, 512, 128), jnp.float32)
CODED = jax.ShapeDtypeStruct((8, 8, 64, 128), jnp.float32)


def sums(*shape):
    return jax.ShapeDtypeStruct(shape, jnp.float32)


def near_own_kernel(place, right, left, col_inv, o_ref):
    def tile(i, carry):
        turn_left(i, right, i, left, col_inv)
        o_ref[tile_rows(i), :] = no_diagonal(i * 128, coherence(i, left, col_inv, both_of(right)))
        return carry

    lax.fori_loop(0, 2, tile, 0)


def near_other_kernel(place, right, left, col_inv, o_ref):
    def tile(i, carry):
        o_ref[tile_rows(i), :] = coherence(i, left, col_inv, both_of(right))
        return carry

    lax.fori_loop(0, 2, tile, 0)


def next_kernel(
    place, own0, other0, right2, near_sums, near_others, unused0, unused1, left, col_inv, o20, o22, o_ref
):
    turn_left(2, right2, 0, left, col_inv)

    def tile(i, carry):
        rows = tile_rows(i)
        put(place, o_ref, i, 0, near_sums[rows, :], near_others[rows, :])
        return carry

    lax.fori_loop(0, 2, tile, 0)
    own = coherence(2, left, col_inv, both_of(own0))
    o20[...] = own
    put(place, o_ref, 2, 0, own, coherence(2, left, col_inv, both_of(other0)))
    o22[...] = no_diagonal(0, coherence(2, left, col_inv, ((right2, 0),)))


def far_own_kernel(
    place, own0, other0, right2, right3, o20, o22, unused0, unused1, unused2, left, col_inv, own_far, o_ref
):
    turn_left(3, right3, 0, left, col_inv)
    own = coherence(3, left, col_inv, both_of(own0))
    put(place, o_ref, 3, 0, own, coherence(3, left, col_inv, both_of(other0)))
    last = no_diagonal(128, coherence(3, left, col_inv, ((right2, 0), (right3, 0))))
    own_far[384:512, :] = last
    own_far[256:384, 0:128] = o22[...]
    own_far[256:384, 128:256] = last[:, :128].T
    for i in range(2):
        lanes = slice(i * 128, (i + 1) * 128)
        own_far[lanes, 0:128] = o20[:, lanes].T
        own_far[lanes, 128:256] = own[:, lanes].T


def far_other_kernel(place, right2, right3, left, col_inv, own_far, unused, o_ref):
    def tile(i, carry):
        other = coherence(i, left, col_inv, ((right2, 0), (right3, 0)))
        put(place, o_ref, i, 1, own_far[tile_rows(i), :], other)
        return carry

    lax.fori_loop(0, 4, tile, 0)


near_own = call(near_own_kernel, 8, [LEFT, COL_INV, sums(256, 256)], products=2)
near_other = call(near_other_kernel, 8, sums(256, 256), products=2)
next_pairs = call(
    next_kernel,
    8,
    [LEFT, COL_INV, sums(128, 256), sums(128, 128), CODED],
    products=3,
    aliases={6: 0, 7: 1},
)
far_own = call(
    far_own_kernel,
    8,
    [LEFT, COL_INV, sums(512, 256), CODED],
    products=3,
    aliases={7: 0, 8: 1, 9: 3},
)
far_other = call(far_other_kernel, 8, CODED, products=4, aliases={6: 0})


def body(scale, coeffs):
    core = lax.axis_index("core")
    chip = lax.axis_index("chip")
    place = jnp.stack((core, chip)).astype(jnp.int32)
    coeffs = pltpu.with_memory_space_constraint(coeffs, pltpu.HBM)
    pieces = [None] * len(STEPS)
    for some in (ORDER[:SPLIT], ORDER[SPLIT:] + (0,)):
        for p, piece in zip(some, turned(place, coeffs, [STEPS[p] for p in some])):
            pieces[p] = piece
    for p in range(1, len(STEPS)):
        pairs = [(c, chip_at(c, STEPS[p], 1)) for c in range(8)]
        pieces[p] = lax.ppermute(pieces[p], "chip", pairs)
    swap = [(0, 1), (1, 0)]
    own0 = arranged(place, *pieces[:4])
    other0 = lax.ppermute(own0, "core", swap)
    left, col_inv, a00 = near_own(place, own0)
    b00 = near_other(place, other0, left, col_inv)
    own2 = arranged(place, *pieces[4:6])
    other2 = lax.ppermute(own2, "core", swap)
    left, col_inv, o20, o22, coded = next_pairs(place, own0, other0, own2, a00, b00, left, col_inv)
    own3 = arranged(place, *pieces[6:])
    other3 = lax.ppermute(own3, "core", swap)
    left, col_inv, own_far, coded = far_own(
        place, own0, other0, own2, own3, o20, o22, left, col_inv, coded
    )
    coded = far_other(place, other2, other3, left, col_inv, own_far, coded)
    coded = coded.reshape(64, 64, 128).astype(jnp.float16)
    coded = lax.all_to_all(coded, ("chip", "band"), 0, 0, tiled=True).astype(jnp.float32)
    square = coded * lax.rsqrt(coded) * (scale / SQUARE**0.5)
    return jnp.sum(jnp.where(coded > 0, square, coded * (-scale / LINEAR)), axis=0)


def solution(mesh):
    fine = Mesh(mesh.devices.reshape(8, 8, 2), ("band", "chip", "core"))
    scale = W * K / 512

    def step(coeffs):
        return body(scale, coeffs)

    return jax.shard_map(
        step,
        mesh=fine,
        in_specs=(P(None, None, ("chip", "core"), "band"),),
        out_specs=P(("chip", "core"), "band"),
        check_vma=False,
    )
```

```python
import jax
import jax.numpy as jnp
from jax import lax
from jax.experimental import pallas as pl
from jax.experimental.pallas import tpu as pltpu
from jax.sharding import Mesh, PartitionSpec as P


K = 8
W = 16
EPS = 1e-06
BANDS = 8

STEPS = ((0, 0), (0, 1), (0, 3), (1, 0), (0, 2), (1, 1), (1, 3), (1, 2))
ORDER = (1, 2, 3, 5, 4, 6, 7)
SPLIT = 3

LIMIT = 2.0**-11
SQUARE = 2.0**8
LINEAR = 2.0**26

WHOLE = pl.BlockSpec(memory_space=pltpu.VMEM)
SCALAR = pl.BlockSpec(memory_space=pltpu.SMEM)
PIECE = (K, BANDS * W, 128)


def chip_at(chip, step, sign):
    half = (chip >> 2) ^ step[0]
    return (half << 2) + ((chip + sign * step[1]) & 3)


def swapped(x):
    return jnp.concatenate((x[:, 64:], x[:, :64]), axis=1)


def call(kernel, mib, out, scratch=(), products=0, aliases=None):
    many = isinstance(out, list)

    def run(place, *args, first=WHOLE):
        return pl.pallas_call(
            kernel,
            in_specs=[SCALAR, first] + [WHOLE] * (len(args) - 1),
            out_specs=[WHOLE] * len(out) if many else WHOLE,
            out_shape=out,
            scratch_shapes=list(scratch),
            input_output_aliases=aliases or {},
            cost_estimate=pl.CostEstimate(
                flops=products * BANDS * 2 * 256**3, bytes_accessed=2**20, transcendentals=0
            ),
            compiler_params=pltpu.CompilerParams(vmem_limit_bytes=mib * 2**20),
        )(place, *args)

    return run


def turn_kernel(steps, place, x_hbm, *refs):
    outs = refs[: len(steps)]
    x_ref, sems = refs[len(steps) :]
    core = place[0]
    chip = place[1]

    def fetch(p):
        lanes = pl.ds(pl.multiple_of(chip_at(chip, steps[p], 1) * 128, 128), 128)
        return pltpu.make_async_copy(x_hbm.at[:, :, :, lanes], x_ref.at[p], sems.at[p])

    for p in range(len(steps)):
        fetch(p).start()
    for p in range(len(steps)):
        fetch(p).wait()

    def step(h, carry):
        for k in range(K // 2):
            for p, o_ref in enumerate(outs):
                first = x_ref[p, core, h * (K // 2) + k]
                second = x_ref[p, 1 - core, h * (K // 2) + k]
                o_ref[h * (K // 2) + k] = jnp.concatenate((first, second), axis=0).T
        return carry

    lax.fori_loop(0, 2, step, 0)


def turned(place, coeffs, steps):
    run = call(
        lambda *refs: turn_kernel(steps, *refs),
        8,
        [jax.ShapeDtypeStruct(PIECE, jnp.bfloat16)] * len(steps),
        (
            pltpu.VMEM((len(steps), 2, K, coeffs.shape[2], 128), jnp.bfloat16),
            pltpu.SemaphoreType.DMA((len(steps),)),
        ),
    )
    return run(place, coeffs, first=pl.BlockSpec(memory_space=pltpu.HBM))


def arrange_kernel(place, *refs):
    *pieces, right = refs
    side = place[0]
    low = lax.broadcasted_iota(jnp.int32, (128, 128), 1) < 64
    row = lax.broadcasted_iota(jnp.int32, (W, 128), 0)
    for m, (a_ref, b_ref) in enumerate(zip(pieces[::2], pieces[1::2])):

        def step(k, power):
            power = list(power)
            a = a_ref[k]
            b = b_ref[k]
            for part, block in (
                (side, jnp.where(low, a, swapped(b))),
                (1 - side, jnp.where(low, swapped(a), b)),
            ):
                for n in range(BANDS):
                    rows = block[n * W : (n + 1) * W]
                    right[n, m, part * K + k] = rows
                    wide = rows.astype(jnp.float32)
                    wide = wide * wide
                    power[n] += wide[:8] + wide[8:]
            return tuple(power)

        power = (jnp.zeros((8, 128), jnp.float32),) * BANDS
        for k in range(K):
            power = step(k, power)
        for n in range(BANDS):
            inv = 1.0 / (jnp.sum(power[n], axis=0, keepdims=True) + EPS)
            high = inv.astype(jnp.bfloat16).astype(jnp.float32)
            middle = (inv - high).astype(jnp.bfloat16).astype(jnp.float32)
            rest = inv - high - middle
            parts = jnp.where(row == 0, high, jnp.where(row == 1, middle, jnp.where(row == 2, rest, 0.0)))
            right[n, m, 2 * K] = parts.astype(jnp.bfloat16)


def arranged(place, *pieces):
    shape = (BANDS, len(pieces) // 2, 2 * K + 1, W, 128)
    return call(arrange_kernel, 8, jax.ShapeDtypeStruct(shape, jnp.bfloat16), products=1)(place, *pieces)


def inverse(right, n, m):
    parts = right[n, m, 2 * K].astype(jnp.float32)
    return jnp.sum(parts, axis=0, keepdims=True)


def columns(right, n, m):
    return right[n, m, 0 : 2 * K].reshape(256, 128)


def tile_rows(i):
    return pl.ds(i * 128 if isinstance(i, int) else pl.multiple_of(i * 128, 128), 128)


def turn_left(i, right, m, left, col_inv):
    rows = tile_rows(i)
    inv = jnp.concatenate([inverse(right, n, m) for n in range(BANDS)], axis=0).T
    for n in range(BANDS):
        block = columns(right, n, m).T
        left[0, n, rows, :] = block[:, :128]
        left[1, n, rows, :] = block[:, 128:]
        left[2, n, rows, :] = -block[:, :128]
        col_inv[n, rows, :] = jnp.broadcast_to(inv[:, n : n + 1], (128, 128))


def coherence(i, left, col_inv, cols):
    rows = tile_rows(i)
    total = jnp.zeros((128, 128 * len(cols)), jnp.float32)
    for n in range(BANDS):
        re = left[0, n, rows, :]
        im = left[1, n, rows, :]
        for_re = jnp.concatenate((re, im), axis=1)
        for_im = jnp.concatenate((im, left[2, n, rows, :]), axis=1)
        lhs = jnp.concatenate((for_re, for_im), axis=0)
        rhs = jnp.concatenate([columns(right, n, m) for right, m in cols], axis=1)
        both = jnp.dot(lhs, rhs, preferred_element_type=jnp.float32)
        re = both[:128]
        im = both[128:]
        ri = jnp.concatenate([inverse(right, n, m) for right, m in cols], axis=1)
        ci = jnp.concatenate([col_inv[n, rows, :]] * len(cols), axis=1)
        total += (re * re + im * im) * ri * ci
    return total


def no_diagonal(first, total):
    row = lax.broadcasted_iota(jnp.int32, total.shape, 0) + first
    col = lax.broadcasted_iota(jnp.int32, total.shape, 1)
    return jnp.where(row == col, 0.0, total)


def put(place, o_ref, i, b, own, other):
    first_core = place[0] == 0
    chip = place[1]
    low = lax.broadcasted_iota(jnp.int32, (128, 128), 1) < 64
    froms = []
    for h in range(2):
        at = chip_at(chip, STEPS[h], -1)
        for t in range(1, 4):
            at = jnp.where(i == t, chip_at(chip, STEPS[2 * t + h], -1), at)
        froms.append(at)
    for m in range(2):
        lanes = slice(m * 128, (m + 1) * 128)
        zero = jnp.where(first_core, own[:, lanes], other[:, lanes])
        one = jnp.where(first_core, other[:, lanes], own[:, lanes])
        for g in range(2):
            if g == 0:
                sums = jnp.where(low, zero, swapped(one))
            else:
                sums = jnp.where(low, swapped(zero), one)
            coded = jnp.where(sums >= LIMIT, sums * sums * SQUARE, sums * -LINEAR)
            to = chip_at(chip, STEPS[4 * b + 2 * m + g], -1)
            for h in range(2):
                o_ref[froms[h], to] = coded[h * 64 : (h + 1) * 64]


def both_of(right):
    return ((right, 0), (right, 1))


LEFT = jax.ShapeDtypeStruct((3, BANDS, 512, 128), jnp.bfloat16)
COL_INV = jax.ShapeDtypeStruct((BANDS, 512, 128), jnp.float32)
CODED = jax.ShapeDtypeStruct((8, 8, 64, 128), jnp.float32)


def sums(*shape):
    return jax.ShapeDtypeStruct(shape, jnp.float32)


def near_own_kernel(place, right, left, col_inv, o_ref):
    def tile(i, carry):
        turn_left(i, right, i, left, col_inv)
        o_ref[tile_rows(i), :] = no_diagonal(i * 128, coherence(i, left, col_inv, both_of(right)))
        return carry

    lax.fori_loop(0, 2, tile, 0)


def near_other_kernel(place, right, left, col_inv, o_ref):
    def tile(i, carry):
        o_ref[tile_rows(i), :] = coherence(i, left, col_inv, both_of(right))
        return carry

    lax.fori_loop(0, 2, tile, 0)


def next_kernel(
    place, own0, other0, right2, near_sums, near_others, unused0, unused1, left, col_inv, o20, o22, o_ref
):
    turn_left(2, right2, 0, left, col_inv)

    def tile(i, carry):
        rows = tile_rows(i)
        put(place, o_ref, i, 0, near_sums[rows, :], near_others[rows, :])
        return carry

    lax.fori_loop(0, 2, tile, 0)
    own = coherence(2, left, col_inv, both_of(own0))
    o20[...] = own
    put(place, o_ref, 2, 0, own, coherence(2, left, col_inv, both_of(other0)))
    o22[...] = no_diagonal(0, coherence(2, left, col_inv, ((right2, 0),)))


def far_own_kernel(
    place, own0, other0, right2, right3, o20, o22, unused0, unused1, unused2, left, col_inv, own_far, o_ref
):
    turn_left(3, right3, 0, left, col_inv)
    own = coherence(3, left, col_inv, both_of(own0))
    put(place, o_ref, 3, 0, own, coherence(3, left, col_inv, both_of(other0)))
    last = no_diagonal(128, coherence(3, left, col_inv, ((right2, 0), (right3, 0))))
    own_far[384:512, :] = last
    own_far[256:384, 0:128] = o22[...]
    own_far[256:384, 128:256] = last[:, :128].T
    for i in range(2):
        lanes = slice(i * 128, (i + 1) * 128)
        own_far[lanes, 0:128] = o20[:, lanes].T
        own_far[lanes, 128:256] = own[:, lanes].T


def far_other_kernel(place, right2, right3, left, col_inv, own_far, unused, o_ref):
    def tile(i, carry):
        other = coherence(i, left, col_inv, ((right2, 0), (right3, 0)))
        put(place, o_ref, i, 1, own_far[tile_rows(i), :], other)
        return carry

    lax.fori_loop(0, 4, tile, 0)


near_own = call(near_own_kernel, 8, [LEFT, COL_INV, sums(256, 256)], products=2)
near_other = call(near_other_kernel, 8, sums(256, 256), products=2)
next_pairs = call(
    next_kernel,
    8,
    [LEFT, COL_INV, sums(128, 256), sums(128, 128), CODED],
    products=3,
    aliases={6: 0, 7: 1},
)
far_own = call(
    far_own_kernel,
    8,
    [LEFT, COL_INV, sums(512, 256), CODED],
    products=3,
    aliases={7: 0, 8: 1, 9: 3},
)
far_other = call(far_other_kernel, 8, CODED, products=4, aliases={6: 0})


def body(scale, coeffs):
    core = lax.axis_index("core")
    chip = lax.axis_index("chip")
    place = jnp.stack((core, chip)).astype(jnp.int32)
    coeffs = pltpu.with_memory_space_constraint(coeffs, pltpu.HBM)
    pieces = [None] * len(STEPS)
    for some in (ORDER[:SPLIT], ORDER[SPLIT:] + (0,)):
        for p, piece in zip(some, turned(place, coeffs, [STEPS[p] for p in some])):
            pieces[p] = piece
    for p in range(1, len(STEPS)):
        pairs = [(c, chip_at(c, STEPS[p], 1)) for c in range(8)]
        pieces[p] = lax.ppermute(pieces[p], "chip", pairs)
    swap = [(0, 1), (1, 0)]
    own0 = arranged(place, *pieces[:4])
    other0 = lax.ppermute(own0, "core", swap)
    left, col_inv, a00 = near_own(place, own0)
    b00 = near_other(place, other0, left, col_inv)
    own2 = arranged(place, *pieces[4:6])
    other2 = lax.ppermute(own2, "core", swap)
    left, col_inv, o20, o22, coded = next_pairs(place, own0, other0, own2, a00, b00, left, col_inv)
    own3 = arranged(place, *pieces[6:])
    other3 = lax.ppermute(own3, "core", swap)
    left, col_inv, own_far, coded = far_own(
        place, own0, other0, own2, own3, o20, o22, left, col_inv, coded
    )
    coded = far_other(place, other2, other3, left, col_inv, own_far, coded)
    coded = coded.reshape(64, 64, 128).astype(jnp.float16)
    coded = lax.all_to_all(coded, ("chip", "band"), 0, 0, tiled=True).astype(jnp.float32)
    value = coded * jnp.where(coded > 0, lax.rsqrt(coded), -(SQUARE**0.5) / LINEAR)
    return jnp.sum(value, axis=0) * (scale / SQUARE**0.5)


def solution(mesh):
    fine = Mesh(mesh.devices.reshape(8, 8, 2), ("band", "chip", "core"))
    scale = W * K / 512

    def step(coeffs):
        return body(scale, coeffs)

    return jax.shard_map(
        step,
        mesh=fine,
        in_specs=(P(None, None, ("chip", "core"), "band"),),
        out_specs=P(("chip", "core"), "band"),
        check_vma=False,
    )
```
